8 devices in a mesh: dp: 2 (over y, z), tp: 4 (over x, core).
Axes of the slice: x: 2, y: 2, z: 1, core: 2. Of those that a mesh axis runs over, the one named last changes fastest.
Arguments:
- x: bfloat16 [4096, 2048], P('dp'), parts along dimension 0
- dy: bfloat16 [4096, 2048], P('dp'), parts along dimension 0
- gate: bfloat16 [4096, 8192], P('dp', 'tp'), parts along dimension 0
- up: bfloat16 [4096, 8192], P('dp', 'tp'), parts along dimension 0
- w_gate: bfloat16 [2048, 8192], P(None, 'tp')
- w_up: bfloat16 [2048, 8192], P(None, 'tp')
- w_down: bfloat16 [8192, 2048], P('tp')
Outputs:
- output 1: bfloat16 [4096, 2048], P('dp'), parts along dimension 0
- output 2: bfloat16 [4096, 8192], P('dp', 'tp'), parts along dimension 0
- output 3: bfloat16 [4096, 8192], P('dp', 'tp'), parts along dimension 0
- output 4: bfloat16 [16384, 2048], P(('dp', 'tp')), parts along dimension 0
There are 2 independent parts. The reference program is written for one: setup_inputs(seed, part) draws one part's arguments, and reference() takes and returns one part's arrays. A program takes and returns all parts, laid end to end along the dimension named above; an argument that names none is the same for every part.
All inputs are finite; a program needn't handle non-finite values.
Results may differ from the reference program's by a relative error of at most 0.012.
Values are sent between devices in bfloat16 or wider.
A program may use at most 2 GiB of HBM per device.

```python
import jax
import jax.numpy as jnp

ROWS = 2048
D = 2048
FF = 8192


def act(gate, up):
    return jax.nn.silu(gate) * up


def setup_inputs(seed: int = 0, part: int = 0) -> dict:
    kx, ky, ka, kb, kg, ku, kd = jax.random.split(jax.random.key(seed), 7)
    kx, ky, ka, kb = (jax.random.fold_in(k, part) for k in (kx, ky, ka, kb))
    drawn = {
        "x": jax.random.normal(kx, (ROWS, D), jnp.float32),
        "dy": jax.random.normal(ky, (ROWS, D), jnp.float32),
        "gate": jax.random.normal(ka, (ROWS, FF), jnp.float32),
        "up": jax.random.normal(kb, (ROWS, FF), jnp.float32),
        "w_gate": jax.random.normal(kg, (D, FF), jnp.float32) * D**-0.5,
        "w_up": jax.random.normal(ku, (D, FF), jnp.float32) * D**-0.5,
        "w_down": jax.random.normal(kd, (FF, D), jnp.float32) * FF**-0.5,
    }
    return {k: v.astype(jnp.bfloat16) for k, v in drawn.items()}


def reference(x, dy, gate, up, w_gate, w_up, w_down):
    hidden, back = jax.vjp(act, gate.astype(jnp.float32), up.astype(jnp.float32))
    d_hidden = jnp.dot(dy, w_down.T, preferred_element_type=jnp.float32)
    d_gate, d_up = (g.astype(jnp.bfloat16) for g in back(d_hidden))
    dx = jnp.dot(d_gate, w_gate.T, preferred_element_type=jnp.float32) + jnp.dot(d_up, w_up.T, preferred_element_type=jnp.float32)
    dw_gate = jnp.dot(x.T, d_gate, preferred_element_type=jnp.float32)
    dw_up = jnp.dot(x.T, d_up, preferred_element_type=jnp.float32)
    dw_down = jnp.dot(hidden.astype(jnp.bfloat16).T, dy, preferred_element_type=jnp.float32)
    return tuple(g.astype(jnp.bfloat16) for g in (dx, dw_gate, dw_up, dw_down))
```

```python
import jax
import jax.numpy as jnp
from jax import lax
from jax.experimental import pallas as pl
from jax.experimental.pallas import tpu as pltpu
from jax.sharding import PartitionSpec as P

ROWS = 2048
D = 2048
F = 2048
R = 256
C = ROWS // R
H = D // 2
NX = 3
LATE = ROWS - NX * R
DONE_AT = {3: 0, 4: 1}
MESH = pl.DeviceIdType.MESH
NT = (((1,), (1,)), ((), ()))
TN = (((0,), (0,)), ((), ()))
BF = jnp.bfloat16


def dot(a, b, dims):
    return lax.dot_general(a, b, dims, preferred_element_type=jnp.float32)


def back_kernel(
    dy, gate, up, wd, wg, wu,
    dg_o, du_o, hid_o, dx_o, late_o,
    wd_v, wgu_v, dy_v, g_v, u_v, acc, dgu_v, hid_v, term_v, got_v, sum_v, cross_v,
    wd_s, wgu_s, in_s, out_s, p1s, p1r, xs, xr, p3s, p3r, f_s, late_s,
):
    me = lax.axis_index("tp")
    core = lax.rem(me, 2)
    partner = me + 1 - 2 * core
    across = lax.rem(me + 2, 4)

    def load(r, slot):
        rows = pl.ds(pl.multiple_of(r * R, R), R)
        return [
            pltpu.make_async_copy(src.at[rows, :], dst.at[slot], in_s.at[slot, k])
            for k, (src, dst) in enumerate(((dy, dy_v), (gate, g_v), (up, u_v)))
        ]

    def store(r, slot):
        rows = pl.ds(pl.multiple_of(r * R, R), R)
        return [
            pltpu.make_async_copy(dgu_v.at[slot, :, pl.ds(0, F)], dg_o.at[rows, :], out_s.at[slot, 0]),
            pltpu.make_async_copy(dgu_v.at[slot, :, pl.ds(F, F)], du_o.at[rows, :], out_s.at[slot, 1]),
            pltpu.make_async_copy(hid_v.at[slot], hid_o.at[rows, :], out_s.at[slot, 2]),
        ]

    def wd_load(n):
        rows = pl.ds(n * (F // 4), F // 4)
        return pltpu.make_async_copy(wd.at[rows, :], wd_v.at[rows, :], wd_s.at[n])

    def wgu_load(half, k):
        rows = pl.ds(pl.multiple_of(half * H, H), H)
        src = (wg, wu)[k]
        return pltpu.make_async_copy(src.at[rows, :], wgu_v.at[rows, pl.ds(k * F, F)], wgu_s.at[half, k])

    def to_partner(r):
        return pltpu.make_async_remote_copy(
            term_v.at[r], got_v.at[r], p1s.at[r], p1r.at[r], device_id={"tp": partner}, device_id_type=MESH)

    def to_across(r):
        return pltpu.make_async_remote_copy(
            sum_v.at[r], cross_v.at[r], xs.at[r], xr.at[r], device_id={"tp": across}, device_id_type=MESH)

    def dx_block(r):
        return dx_o.at[pl.ds(r * R, R), pl.ds(pl.multiple_of(core * H, H), H)]

    def share(r):
        return pltpu.make_async_remote_copy(
            sum_v.at[r], dx_block(r), p3s.at[r], p3r.at[r], device_id={"tp": partner}, device_id_type=MESH)

    def keep(r):
        return pltpu.make_async_copy(sum_v.at[r], dx_block(r), f_s.at[r])

    def put_late(r):
        rows = pl.ds(pl.multiple_of((r - NX) * R, R), R)
        return pltpu.make_async_copy(sum_v.at[r], late_o.at[rows, :], late_s.at[r])

    def epilogue(slot, out):
        for i in range(0, R, 16):
            for j in range(0, F, 512):
                at = (pl.ds(i, 16), pl.ds(j, 512))
                dh = acc[at]
                g = g_v[(slot, *at)].astype(jnp.float32)
                u = u_v[(slot, *at)].astype(jnp.float32)
                sig = 1.0 / (1.0 + jnp.exp(-g))
                silu = g * sig
                hid_v[(out, *at)] = (silu * u).astype(BF)
                dgu_v[(out, pl.ds(i, 16), pl.ds(j, 512))] = ((dh * u) * (sig * (1.0 + g * (1.0 - sig)))).astype(BF)
                dgu_v[(out, pl.ds(i, 16), pl.ds(F + j, 512))] = (dh * silu).astype(BF)

    def term(slot, half):
        rows = pl.ds(pl.multiple_of(half * H, H), H)
        return dot(dgu_v[slot], wgu_v[rows, :], NT)

    def finish(r):
        to_across(r).wait()
        sum_v[r] = (sum_v[r].astype(jnp.float32) + cross_v[r].astype(jnp.float32)).astype(BF)
        share(r).start()
        keep(r).start()

    for c in load(0, 0)[:1] + [wd_load(n) for n in range(4)] + load(0, 0)[1:]:
        c.start()
    barrier = pltpu.get_barrier_semaphore()
    for other in (partner, across):
        pl.semaphore_signal(barrier, inc=1, device_id={"tp": other}, device_id_type=MESH)
    pl.semaphore_wait(barrier, 2)

    load(0, 0)[0].wait()
    for n in range(4):
        wd_load(n).wait()
        if n == 2:
            for k in range(2):
                wgu_load(1 - core, k).start()
        if n == 3:
            for c in load(1, 1):
                c.start()
            for k in range(2):
                wgu_load(core, k).start()
        acc[:, pl.ds(n * 512, 512)] = dot(dy_v[0], wd_v[pl.ds(n * 512, 512), :], NT)
    for c in load(0, 0)[1:]:
        c.wait()
    epilogue(0, 0)
    for c in store(0, 0) + load(2, 0):
        c.start()
    for c in load(1, 1):
        c.wait()
    acc[...] = dot(dy_v[1], wd_v[...], NT)
    epilogue(1, 1)
    for c in store(1, 1) + load(3, 1):
        c.start()
    for k in range(2):
        wgu_load(1 - core, k).wait()
    term_v[0] = term(0, 1 - core).astype(BF)
    to_partner(0).start()
    for k in range(2):
        wgu_load(core, k).wait()

    def step(r, _):
        new, slot = lax.rem(r + 2, 3), lax.rem(r, 2)
        for c in load(r + 2, slot):
            c.wait()

        @pl.when(r >= 1)
        def _():
            for c in store(r - 1, new):
                c.wait()

        acc[...] = dot(dy_v[slot], wd_v[...], NT)
        to_partner(r).wait_recv()
        sum_v[r] = (term(lax.rem(r, 3), core) + got_v[r].astype(jnp.float32)).astype(BF)
        epilogue(slot, new)
        term_v[r + 1] = term(lax.rem(r + 1, 3), 1 - core).astype(BF)
        to_partner(r + 1).start()

        @pl.when(r < NX)
        def _():
            to_across(r).start()

        @pl.when(r >= NX)
        def _():
            put_late(r).start()

        for c in store(r + 2, new):
            c.start()

        @pl.when(r + 4 < C)
        def _():
            for c in load(r + 4, slot):
                c.start()

        for at, q in DONE_AT.items():
            @pl.when(r == at)
            def _():
                finish(q)
        return 0

    lax.fori_loop(0, C - 2, step, 0)

    r = C - 2
    to_partner(r).wait_recv()
    sum_v[r] = (term(r % 3, core) + got_v[r].astype(jnp.float32)).astype(BF)
    term_v[r + 1] = term((r + 1) % 3, 1 - core).astype(BF)
    to_partner(r + 1).start()
    put_late(r).start()
    for q in range(NX):
        if q not in DONE_AT.values():
            finish(q)
    r = C - 1
    to_partner(r).wait_recv()
    sum_v[r] = (term(r % 3, core) + got_v[r].astype(jnp.float32)).astype(BF)
    put_late(r).start()

    for q in range(NX):
        share(q).wait()
        keep(q).wait()
    for q in range(NX, C):
        put_late(q).wait()
    for q in range(C):
        to_partner(q).wait_send()
    for q in range(C - 3, C):
        for c in store(q, q % 3):
            c.wait()


def back(dy, gate, up, wd, wg, wu):
    hbm = pl.BlockSpec(memory_space=pl.ANY)
    full = jax.ShapeDtypeStruct((ROWS, F), BF)
    dma = pltpu.SemaphoreType.DMA
    return pl.pallas_call(
        back_kernel,
        in_specs=[hbm] * 6,
        out_specs=[hbm] * 5,
        out_shape=[full, full, full, jax.ShapeDtypeStruct((NX * R, D), BF), jax.ShapeDtypeStruct((LATE, H), BF)],
        scratch_shapes=[
            pltpu.VMEM((F, D), BF),
            pltpu.VMEM((D, 2 * F), BF),
            pltpu.VMEM((2, R, D), BF),
            pltpu.VMEM((2, R, F), BF),
            pltpu.VMEM((2, R, F), BF),
            pltpu.VMEM((R, F), jnp.float32),
            pltpu.VMEM((3, R, 2 * F), BF),
            pltpu.VMEM((3, R, F), BF),
            pltpu.VMEM((C, R, H), BF),
            pltpu.VMEM((C, R, H), BF),
            pltpu.VMEM((C, R, H), BF),
            pltpu.VMEM((NX, R, H), BF),
            dma((4,)), dma((2, 2)), dma((2, 3)), dma((3, 3)), dma((C,)), dma((C,)), dma((NX,)), dma((NX,)),
            dma((NX,)), dma((NX,)), dma((NX,)), dma((C,)),
        ],
        compiler_params=pltpu.CompilerParams(collective_id=0, has_side_effects=True, vmem_limit_bytes=66_900_000),
        cost_estimate=pl.CostEstimate(flops=6 * ROWS * D * F, bytes_accessed=90_000_000, transcendentals=ROWS * F),
        name="back",
    )(dy, gate, up, wd, wg, wu)


B = 1024
FIRST = {0: (0, 2), 1: (3,), 2: (1,), 4: (4,), 5: (5,), 8: (6, 8), 9: (9,), 10: (7,)}


def weights_kernel(x, dg, du, hid, dy, dx_e, dwg, dwu, dwd, dx_o, panel, out, early, panel_s, out_s, early_s):
    arrays = (x, dg, du, hid, dy)

    def panel_load(p):
        return pltpu.make_async_copy(arrays[p // 2].at[:, pl.ds((p % 2) * B, B)], panel.at[p], panel_s.at[p])

    def put(t, slot, ref):
        i, j = lax.rem(t, 4) // 2, lax.rem(t, 2)
        at = ref.at[pl.ds(pl.multiple_of(i * B, B), B), pl.ds(pl.multiple_of(j * B, B), B)]
        return pltpu.make_async_copy(out.at[slot], at, out_s.at[slot])

    def take():
        return pltpu.make_async_copy(dx_e, early, early_s.at[0])

    def give():
        return pltpu.make_async_copy(early, dx_o.at[pl.ds(0, NX * R), :], early_s.at[1])

    for p in FIRST[0]:
        panel_load(p).start()

    def step(t, _):
        for at, ps in FIRST.items():
            @pl.when(t == at)
            def _():
                for p in ps:
                    panel_load(p).wait()

            if at:
                @pl.when(t == max(at - 2, 0))
                def _():
                    for p in ps:
                        panel_load(p).start()

        @pl.when(t == 4)
        def _():
            take().start()

        @pl.when(t == 6)
        def _():
            take().wait()
            give().start()

        slot = lax.rem(t, 2)

        @pl.when(t >= 2)
        def _():
            put(t, slot, dwg).wait()

        left = t // 8 * 6 + lax.rem(t, 4) // 2
        right = 2 + t // 4 * 2 + t // 8 * 2 + lax.rem(t, 2)
        out[slot] = dot(panel[left], panel[right], TN).astype(BF)
        for k, ref in enumerate((dwg, dwu, dwd)):
            @pl.when(t // 4 == k)
            def _():
                put(t, slot, ref).start()
        return 0

    lax.fori_loop(0, 12, step, 0)
    put(10, 0, dwd).wait()
    put(11, 1, dwd).wait()
    give().wait()


def weights(x, dg, du, hid, dy, dx_e):
    hbm = pl.BlockSpec(memory_space=pl.ANY)
    full = jax.ShapeDtypeStruct((ROWS, F), BF)
    dma = pltpu.SemaphoreType.DMA
    return pl.pallas_call(
        weights_kernel,
        in_specs=[hbm] * 6,
        out_specs=[hbm] * 4,
        out_shape=[full] * 4,
        scratch_shapes=[
            pltpu.VMEM((10, ROWS, B), BF),
            pltpu.VMEM((2, B, B), BF),
            pltpu.VMEM((NX * R, D), BF),
            dma((10,)), dma((2,)), dma((2,)),
        ],
        compiler_params=pltpu.CompilerParams(vmem_limit_bytes=66_900_000),
        cost_estimate=pl.CostEstimate(flops=6 * ROWS * D * F, bytes_accessed=70_000_000, transcendentals=0),
        name="weights",
    )(x, dg, du, hid, dy, dx_e)


def join_kernel(mine, theirs, dx_in, dx_o):
    core = lax.rem(lax.axis_index("tp"), 2)
    a, b = mine[...], theirs[...]
    dx_o[:, pl.ds(0, H)] = jnp.where(core == 0, a, b)
    dx_o[:, pl.ds(H, H)] = jnp.where(core == 0, b, a)


def join(mine, theirs, dx):
    half = pl.BlockSpec((R, H), lambda i: (i, 0))
    return pl.pallas_call(
        join_kernel,
        grid=(C - NX,),
        in_specs=[half, half, pl.BlockSpec(memory_space=pl.ANY)],
        out_specs=pl.BlockSpec((R, D), lambda i: (i + NX, 0)),
        out_shape=jax.ShapeDtypeStruct((ROWS, D), BF),
        input_output_aliases={2: 0},
        name="join",
    )(mine, theirs, dx)


def solution(mesh):
    def step(x, dy, gate, up, w_gate, w_up, w_down):
        dg, du, hid, dx_e, late = back(dy, gate, up, w_down, w_gate, w_up)
        crossed = lax.ppermute(late, "tp", [(i, i ^ 2) for i in range(4)])
        dwg, dwu, dwd, dx = weights(x, dg, du, hid, dy, dx_e)
        crossed, dx = lax.optimization_barrier((crossed, dx))
        mine = (late.astype(jnp.float32) + crossed.astype(jnp.float32)).astype(BF)
        theirs = lax.ppermute(mine, "tp", [(i, i ^ 1) for i in range(4)])
        return join(mine, theirs, dx), dwg, dwu, dwd

    tokens, columns, rows = P("dp", None), P(None, "tp"), P("tp", None)
    return jax.shard_map(
        step,
        mesh=mesh,
        in_specs=(tokens, tokens, P("dp", "tp"), P("dp", "tp"), columns, columns, rows),
        out_specs=(tokens, P("dp", "tp"), P("dp", "tp"), P(("dp", "tp"), None)),
        check_vma=False,
    )
```

```python
import jax
import jax.numpy as jnp
from jax import lax
from jax.experimental import pallas as pl
from jax.experimental.pallas import tpu as pltpu
from jax.sharding import PartitionSpec as P

ROWS = 2048
D = 2048
F = 2048
R = 256
C = ROWS // R
H = D // 2
NX = 3
LATE = ROWS - NX * R
DONE_AT = {3: 0, 4: 1}
FLAGS = {}
MESH = pl.DeviceIdType.MESH
NT = (((1,), (1,)), ((), ()))
TN = (((0,), (0,)), ((), ()))
BF = jnp.bfloat16


def dot(a, b, dims):
    return lax.dot_general(a, b, dims, preferred_element_type=jnp.float32)


def back_kernel(
    dy, gate, up, wd, wg, wu,
    dg_o, du_o, hid_o, dx_o, late_o,
    wd_v, wgu_v, dy_v, g_v, u_v, acc, half, dgu_a, dgu_b, hid_a, hid_b, term_v, got_v, sum_v, cross_v,
    wd_s, wgu_s, in_s, out_s, p1s, p1r, xs, xr, p3s, p3r, f_s, late_s,
):
    me = lax.axis_index("tp")
    core = lax.rem(me, 2)
    partner = me + 1 - 2 * core
    across = lax.rem(me + 2, 4)
    dgu_v, hid_v = (dgu_a, dgu_b), (hid_a, hid_b)

    def load(r, slot):
        rows = pl.ds(pl.multiple_of(r * R, R), R)
        return [
            pltpu.make_async_copy(src.at[rows, :], dst.at[slot], in_s.at[slot, k])
            for k, (src, dst) in enumerate(((dy, dy_v), (gate, g_v), (up, u_v)))
        ]

    def store(r, slot):
        rows = pl.ds(pl.multiple_of(r * R, R), R)
        return [
            pltpu.make_async_copy(dgu_v[slot].at[:, pl.ds(0, F)], dg_o.at[rows, :], out_s.at[slot, 0]),
            pltpu.make_async_copy(dgu_v[slot].at[:, pl.ds(F, F)], du_o.at[rows, :], out_s.at[slot, 1]),
            pltpu.make_async_copy(hid_v[slot], hid_o.at[rows, :], out_s.at[slot, 2]),
        ]

    def wd_load(n):
        rows = pl.ds(pl.multiple_of(n * (F // 4), F // 4), F // 4)
        return pltpu.make_async_copy(wd.at[rows, :], wd_v.at[rows, :], wd_s.at[n])

    def wgu_load(side, k):
        rows = pl.ds(pl.multiple_of(side * H, H), H)
        src = (wg, wu)[k]
        return pltpu.make_async_copy(src.at[rows, :], wgu_v.at[rows, pl.ds(k * F, F)], wgu_s.at[side, k])

    def to_partner(r):
        return pltpu.make_async_remote_copy(
            term_v.at[lax.rem(r, 2)], got_v.at[lax.rem(r, 4)], p1s.at[r], p1r.at[r], device_id={"tp": partner}, device_id_type=MESH)

    def to_across(r):
        return pltpu.make_async_remote_copy(
            sum_v.at[r], cross_v.at[r], xs.at[r], xr.at[r], device_id={"tp": across}, device_id_type=MESH)

    def dx_block(r):
        return dx_o.at[pl.ds(r * R, R), pl.ds(pl.multiple_of(core * H, H), H)]

    def share(r):
        return pltpu.make_async_remote_copy(
            sum_v.at[r], dx_block(r), p3s.at[r], p3r.at[r], device_id={"tp": partner}, device_id_type=MESH)

    def keep(r):
        return pltpu.make_async_copy(sum_v.at[r], dx_block(r), f_s.at[r])

    def put_late(r):
        rows = pl.ds(pl.multiple_of((r - NX) * R, R), R)
        return pltpu.make_async_copy(sum_v.at[r], late_o.at[rows, :], late_s.at[r])

    def epilogue(slot):
        for i in range(0, R, 16):
            for j in range(0, F, 512):
                at = (pl.ds(i, 16), pl.ds(j, 512))
                dh = acc[at]
                g = g_v[(slot, *at)].astype(jnp.float32)
                u = u_v[(slot, *at)].astype(jnp.float32)
                sig = 1.0 / (1.0 + jnp.exp(-g))
                silu = g * sig
                hid_v[slot][at] = (silu * u).astype(BF)
                dgu_v[slot][at] = ((dh * u) * (sig * (1.0 + g * (1.0 - sig)))).astype(BF)
                dgu_v[slot][pl.ds(i, 16), pl.ds(F + j, 512)] = (dh * silu).astype(BF)

    def term(slot, side):
        rows = pl.ds(pl.multiple_of(side * H, H), H)
        return dot(dgu_v[slot][...], wgu_v[rows, :], NT)

    def add(r):
        to_partner(r).wait_recv()
        sum_v[r] = (half[...] + got_v[lax.rem(r, 4)].astype(jnp.float32)).astype(BF)

    def other(r, slot):
        term_v[slot] = term(slot, 1 - core).astype(BF)

    def finish(r):
        to_across(r).wait()
        sum_v[r] = (sum_v[r].astype(jnp.float32) + cross_v[r].astype(jnp.float32)).astype(BF)
        share(r).start()
        keep(r).start()

    def run(copies, act):
        for c in copies:
            getattr(c, act)()

    run(load(0, 0)[:1] + [wd_load(n) for n in range(4)] + load(1, 1)[:1] + load(0, 0)[1:], "start")
    barrier = pltpu.get_barrier_semaphore()
    for peer in (partner, across):
        pl.semaphore_signal(barrier, inc=1, device_id={"tp": peer}, device_id_type=MESH)

    load(0, 0)[0].wait()

    def quarter(n, _):
        wd_load(n).wait()

        @pl.when(n == 1)
        def _():
            run([wgu_load(1 - core, k) for k in range(2)], "start")

        at = pl.ds(pl.multiple_of(n * (F // 4), F // 4), F // 4)
        acc[:, at] = dot(dy_v[0], wd_v[at, :], NT)
        return 0

    lax.fori_loop(0, 4, quarter, 0)
    run(load(0, 0)[1:], "wait")
    run(load(1, 1)[1:], "start")
    epilogue(0)
    run([wgu_load(core, k) for k in range(2)] + store(0, 0) + load(2, 0), "start")
    run([wgu_load(1 - core, k) for k in range(2)], "wait")
    other(0, 0)
    pl.semaphore_wait(barrier, 2)
    to_partner(0).start()

    def step(r, cur):
        new = 1 - cur
        run(load(r + 1, new), "wait")

        @pl.when(r >= 1)
        def _():
            run(store(r - 1, new), "wait")
            to_partner(r - 1).wait_send()

        @pl.when(r == 0)
        def _():
            run([wgu_load(core, k) for k in range(2)], "wait")

        acc[...] = dot(dy_v[new], wd_v[...], NT)
        half[...] = term(cur, core)
        epilogue(new)
        other(r + 1, new)
        to_partner(r + 1).start()
        add(r)

        @pl.when(r < NX)
        def _():
            to_across(r).start()

        @pl.when(r >= NX)
        def _():
            put_late(r).start()

        run(store(r + 1, new), "start")

        @pl.when(r + 3 < C)
        def _():
            run(load(r + 3, new), "start")

        for at, q in DONE_AT.items():
            @pl.when(r == at)
            def _():
                finish(q)

    def pair(p, _):
        step(2 * p, 0)
        step(2 * p + 1, 1)
        return 0

    lax.fori_loop(0, C // 2 - 1, pair, 0)
    step(C - 2, 0)
    r = C - 1
    half[...] = term(1, core)
    add(r)
    put_late(r).start()
    for q in range(NX):
        if q not in DONE_AT.values():
            finish(q)

    for q in range(NX):
        share(q).wait()
        keep(q).wait()
    for q in range(NX, C):
        put_late(q).wait()
    for q in range(C - 2, C):
        to_partner(q).wait_send()
    for q in range(C - 2, C):
        run(store(q, q % 2), "wait")


def back(dy, gate, up, wd, wg, wu):
    hbm = pl.BlockSpec(memory_space=pl.ANY)
    full = jax.ShapeDtypeStruct((ROWS, F), BF)
    dma = pltpu.SemaphoreType.DMA
    return pl.pallas_call(
        back_kernel,
        in_specs=[hbm] * 6,
        out_specs=[hbm] * 5,
        out_shape=[full, full, full, jax.ShapeDtypeStruct((NX * R, D), BF), jax.ShapeDtypeStruct((LATE, H), BF)],
        scratch_shapes=[
            pltpu.VMEM((F, D), BF),
            pltpu.VMEM((D, 2 * F), BF),
            pltpu.VMEM((2, R, D), BF),
            pltpu.VMEM((2, R, F), BF),
            pltpu.VMEM((2, R, F), BF),
            pltpu.VMEM((R, F), jnp.float32),
            pltpu.VMEM((R, H), jnp.float32),
            pltpu.VMEM((R, 2 * F), BF),
            pltpu.VMEM((R, 2 * F), BF),
            pltpu.VMEM((R, F), BF),
            pltpu.VMEM((R, F), BF),
            pltpu.VMEM((2, R, H), BF),
            pltpu.VMEM((4, R, H), BF),
            pltpu.VMEM((C, R, H), BF),
            pltpu.VMEM((NX, R, H), BF),
            dma((4,)), dma((2, 2)), dma((2, 3)), dma((2, 3)), dma((C,)), dma((C,)), dma((NX,)), dma((NX,)),
            dma((NX,)), dma((NX,)), dma((NX,)), dma((C,)),
        ],
        compiler_params=pltpu.CompilerParams(collective_id=0, has_side_effects=True, vmem_limit_bytes=66_900_000, flags=FLAGS),
        cost_estimate=pl.CostEstimate(flops=6 * ROWS * D * F, bytes_accessed=90_000_000, transcendentals=ROWS * F),
        name="back",
    )(dy, gate, up, wd, wg, wu)


B = 1024
FIRST = {0: (0, 2), 1: (3,), 2: (1,), 4: (4,), 5: (5,), 8: (6, 8), 9: (9,), 10: (7,)}


def weights_kernel(x, dg, du, hid, dy, dx_e, dwg, dwu, dwd, dx_o, panel, out, early, panel_s, out_s, early_s):
    arrays = (x, dg, du, hid, dy)

    def panel_load(p):
        return pltpu.make_async_copy(arrays[p // 2].at[:, pl.ds((p % 2) * B, B)], panel.at[p], panel_s.at[p])

    def put(t, slot, ref):
        i, j = lax.rem(t, 4) // 2, lax.rem(t, 2)
        at = ref.at[pl.ds(pl.multiple_of(i * B, B), B), pl.ds(pl.multiple_of(j * B, B), B)]
        return pltpu.make_async_copy(out.at[slot], at, out_s.at[slot])

    def take():
        return pltpu.make_async_copy(dx_e, early, early_s.at[0])

    def give():
        return pltpu.make_async_copy(early, dx_o.at[pl.ds(0, NX * R), :], early_s.at[1])

    for p in FIRST[0]:
        panel_load(p).start()

    def step(t, _):
        for at, ps in FIRST.items():
            @pl.when(t == at)
            def _():
                for p in ps:
                    panel_load(p).wait()

            if at:
                @pl.when(t == max(at - 2, 0))
                def _():
                    for p in ps:
                        panel_load(p).start()

        @pl.when(t == 4)
        def _():
            take().start()

        @pl.when(t == 6)
        def _():
            take().wait()
            give().start()

        slot = lax.rem(t, 2)

        @pl.when(t >= 2)
        def _():
            put(t, slot, dwg).wait()

        left = t // 8 * 6 + lax.rem(t, 4) // 2
        right = 2 + t // 4 * 2 + t // 8 * 2 + lax.rem(t, 2)
        out[slot] = dot(panel[left], panel[right], TN).astype(BF)
        for k, ref in enumerate((dwg, dwu, dwd)):
            @pl.when(t // 4 == k)
            def _():
                put(t, slot, ref).start()
        return 0

    lax.fori_loop(0, 12, step, 0)
    put(10, 0, dwd).wait()
    put(11, 1, dwd).wait()
    give().wait()


def weights(x, dg, du, hid, dy, dx_e):
    hbm = pl.BlockSpec(memory_space=pl.ANY)
    full = jax.ShapeDtypeStruct((ROWS, F), BF)
    dma = pltpu.SemaphoreType.DMA
    return pl.pallas_call(
        weights_kernel,
        in_specs=[hbm] * 6,
        out_specs=[hbm] * 4,
        out_shape=[full] * 4,
        scratch_shapes=[
            pltpu.VMEM((10, ROWS, B), BF),
            pltpu.VMEM((2, B, B), BF),
            pltpu.VMEM((NX * R, D), BF),
            dma((10,)), dma((2,)), dma((2,)),
        ],
        compiler_params=pltpu.CompilerParams(vmem_limit_bytes=66_900_000),
        cost_estimate=pl.CostEstimate(flops=6 * ROWS * D * F, bytes_accessed=70_000_000, transcendentals=0),
        name="weights",
    )(x, dg, du, hid, dy, dx_e)


def join_kernel(sum_m, sum_p, far_m, far_p, dx_in, dx_o, part, out, part_s, out_s):
    core = lax.rem(lax.axis_index("tp"), 2)
    n = C - NX

    def load(i, k):
        src = (sum_m, far_m, sum_p, far_p)[k]
        return pltpu.make_async_copy(src.at[pl.ds(i * R, R), :], part.at[i, k], part_s.at[i, k])

    def put(i, k):
        columns = pl.ds(pl.multiple_of((core * (1 - k) + (1 - core) * k) * H, H), H)
        return pltpu.make_async_copy(out.at[i, k], dx_o.at[pl.ds((i + NX) * R, R), columns], out_s.at[i, k])

    for i in range(n):
        for k in range(4):
            load(i, k).start()
    for i in range(n):
        for k in range(2):
            load(i, 2 * k).wait()
            load(i, 2 * k + 1).wait()
            out[i, k] = (part[i, 2 * k].astype(jnp.float32) + part[i, 2 * k + 1].astype(jnp.float32)).astype(BF)
            put(i, k).start()
    for i in range(n):
        for k in range(2):
            put(i, k).wait()


def join(sum_m, sum_p, far_m, far_p, dx):
    hbm = pl.BlockSpec(memory_space=pl.ANY)
    n = C - NX
    dma = pltpu.SemaphoreType.DMA
    return pl.pallas_call(
        join_kernel,
        in_specs=[hbm] * 5,
        out_specs=hbm,
        out_shape=jax.ShapeDtypeStruct((ROWS, D), BF),
        scratch_shapes=[pltpu.VMEM((n, 4, R, H), BF), pltpu.VMEM((n, 2, R, H), BF), dma((n, 4)), dma((n, 2))],
        input_output_aliases={4: 0},
        compiler_params=pltpu.CompilerParams(vmem_limit_bytes=66_900_000),
        name="join",
    )(sum_m, sum_p, far_m, far_p, dx)


def solution(mesh):
    def step(x, dy, gate, up, w_gate, w_up, w_down):
        dg, du, hid, dx_e, late = back(dy, gate, up, w_down, w_gate, w_up)
        across = [(i, i ^ 2) for i in range(4)]
        partner = [(i, i ^ 1) for i in range(4)]
        far = lax.ppermute(late, "tp", across)
        late_p = lax.ppermute(late, "tp", partner)
        dwg, dwu, dwd, dx = weights(x, dg, du, hid, dy, dx_e)
        far, late_p, dx = lax.optimization_barrier((far, late_p, dx))
        far_p = lax.ppermute(far, "tp", partner)
        return join(late, late_p, far, far_p, dx), dwg, dwu, dwd

    tokens, columns, rows = P("dp", None), P(None, "tp"), P("tp", None)
    return jax.shard_map(
        step,
        mesh=mesh,
        in_specs=(tokens, tokens, P("dp", "tp"), P("dp", "tp"), columns, columns, rows),
        out_specs=(tokens, P("dp", "tp"), P("dp", "tp"), P(("dp", "tp"), None)),
        check_vma=False,
    )
```
